32 devices in a mesh: dp: 4 (over y, x), mp: 8 (over z, core).
Axes of the slice: x: 2, y: 2, z: 4, core: 2. Of those that a mesh axis runs over, the one named last changes fastest.
Arguments:
- query_grads: bfloat16 [4, 1, 3584, 4096], P('dp', None, None, 'mp'), may hold values from -102 to 102
- merge_grads: bfloat16 [4, 1, 4096, 3584], P('dp', None, 'mp'), may hold values from -102 to 102
- query_accum: float32 [1, 3584, 4096], P(None, 'dp', 'mp'), may hold values from -406 to 406
- merge_accum: float32 [1, 4096, 3584], P(None, 'mp', 'dp'), may hold values from -406 to 406
- query_master: float32 [1, 3584, 4096], P(None, 'dp', 'mp'), may hold values from -0.75 to 0.75
- merge_master: float32 [1, 4096, 3584], P(None, 'mp', 'dp'), may hold values from -0.75 to 0.75
- query_moment: float32 [1, 3584, 4096], P(None, 'dp', 'mp'), may hold values from -6 to 6
- merge_moment: float32 [1, 4096, 3584], P(None, 'mp', 'dp'), may hold values from -6 to 6
- query_second: float32 [1, 3584, 4096], P(None, 'dp', 'mp'), may hold values from 0.3 to 3
- merge_second: float32 [1, 4096, 3584], P(None, 'mp', 'dp'), may hold values from 0.3 to 3
Outputs:
- query_weight: bfloat16 [1, 3584, 4096], P(None, None, 'mp')
- merge_weight: bfloat16 [1, 4096, 3584], P(None, 'mp')
- query_shard: float32 [1, 3584, 4096], P(None, 'dp', 'mp')
- merge_shard: float32 [1, 4096, 3584], P(None, 'mp', 'dp')
- query_first: float32 [1, 3584, 4096], P(None, 'dp', 'mp')
- merge_first: float32 [1, 4096, 3584], P(None, 'mp', 'dp')
- query_variance: float32 [1, 3584, 4096], P(None, 'dp', 'mp')
- merge_variance: float32 [1, 4096, 3584], P(None, 'mp', 'dp')
The draws below stay inside these ranges and needn't reach their ends.
All inputs are finite; a program needn't handle non-finite values.
Results may differ from the reference program's by a relative error of at most 0.0015.
Values may be sent and summed in bfloat16 or wider, within the bound.
A program may use at most 128 MiB of HBM per device.

```python
import math
import jax
import jax.numpy as jnp
from jax import lax

D = 3584
HEADS = 16
HEAD_DIM = 256
LAYERS = 1
STEP = 10
QW = 4096
ENTRIES = 29360128
N_DP = 4


def scaled_field(key, tag, noise_tag, shape, base):
    rows = shape[-2]
    cols = shape[-1]
    scale_key = jax.random.fold_in(key, tag)
    row_rise = 1.0 + 0.75 * jnp.arange(rows, dtype=jnp.float32)[:, None] / rows
    col_rise = 1.0 + 0.75 * jnp.arange(cols, dtype=jnp.float32)[None, :] / cols
    row_shape = tuple(shape[:-1]) + (1,)
    col_shape = tuple(shape[:-2]) + (1, cols)
    row_scale = jnp.exp(jax.random.uniform(jax.random.fold_in(scale_key, 1), row_shape, jnp.float32) * math.log(10.0)) * row_rise
    col_scale = jnp.exp(jax.random.uniform(jax.random.fold_in(scale_key, 2), col_shape, jnp.float32) * math.log(10.0)) * col_rise
    noise_key = jax.random.fold_in(key, noise_tag)
    value = jax.random.truncated_normal(noise_key, -4.0, 4.0, shape, jnp.float32)
    return base * value * row_scale * col_scale


def draw_query_grads(key, part):
    return scaled_field(key, 1, 5, (N_DP, LAYERS, D, HEADS * HEAD_DIM), 0.05).astype(jnp.bfloat16)


def draw_merge_grads(key, part):
    return scaled_field(key, 2, 6, (N_DP, LAYERS, HEADS * HEAD_DIM, D), 0.05).astype(jnp.bfloat16)


def draw_query_accum(key, part):
    return scaled_field(key, 3, 7, (LAYERS, D, HEADS * HEAD_DIM), 0.2)


def draw_merge_accum(key, part):
    return scaled_field(key, 4, 8, (LAYERS, HEADS * HEAD_DIM, D), 0.2)


def block_scale(key, extent, split, smallest, largest):
    level, own = 1.0, jax.random.fold_in(key, 6)
    for position, parts in split:
        draws = jnp.exp(jax.random.uniform(jax.random.fold_in(own, position), (parts,), jnp.float32, smallest / len(split), largest / len(split)))
        level = level * jnp.repeat(draws, extent[position] // parts).reshape([-1 if axis == position else 1 for axis in range(len(extent))])
    return level


def bell_draw(rng, shape, scale, most, pieces=(), kind=jnp.bfloat16):
    drawn = jax.random.normal(rng, shape, jnp.float32) * scale
    if len(pieces) > 0:
        drawn = block_scale(rng, shape, pieces, -0.22, 0.18) * drawn
    return jnp.clip(drawn, min=-most, max=most).astype(kind)


def setup_inputs(seed: int = 0) -> dict:
    key_of = jax.random.split(jax.random.key(seed), 11)
    return {
        "query_grads": draw_query_grads(jax.random.fold_in(key_of[10], 71), 0),
        "merge_grads": draw_merge_grads(jax.random.fold_in(key_of[10], 71), 0),
        "query_accum": draw_query_accum(jax.random.fold_in(key_of[10], 71), 0),
        "merge_accum": draw_merge_accum(jax.random.fold_in(key_of[10], 71), 0),
        "query_master": bell_draw(key_of[4], (LAYERS, D, QW), 0.05, 0.75, ((1, 4), (2, 8)), jnp.float32),
        "merge_master": bell_draw(key_of[5], (LAYERS, QW, D), 0.05, 0.75, ((1, 8), (2, 4)), jnp.float32),
        "query_moment": bell_draw(key_of[6], (LAYERS, D, QW), 1.0, 6.0, ((1, 4), (2, 8)), jnp.float32),
        "merge_moment": bell_draw(key_of[7], (LAYERS, QW, D), 1.0, 6.0, ((1, 8), (2, 4)), jnp.float32),
        "query_second": jnp.clip(jnp.exp(math.log(3.0) - 2.3025851 * jax.random.uniform(key_of[8], (LAYERS, D, QW), jnp.float32) ** block_scale(key_of[8], (LAYERS, D, QW), ((1, 4), (2, 8)), -0.2, 0.2)), 0.3, 3.0),
        "merge_second": jnp.clip(jnp.exp(math.log(3.0) - 2.3025851 * jax.random.uniform(key_of[9], (LAYERS, QW, D), jnp.float32) ** block_scale(key_of[9], (LAYERS, QW, D), ((1, 8), (2, 4)), -0.2, 0.2)), 0.3, 3.0),
    }


beta_one = 0.9
beta_two = 0.95
learn_rate = 0.002
weight_decay = 0.1
adam_eps = 1e-08

def adamw(total, clip, master, moment, second):
    scaled = clip * total
    first = beta_one * moment + (1.0 - beta_one) * scaled
    variance = beta_two * second + (1.0 - beta_two) * scaled * scaled
    corr_one = 1.0 - beta_one ** STEP
    corr_two = 1.0 - beta_two ** STEP
    update = first / corr_one / (jnp.sqrt(variance / corr_two) + adam_eps) + weight_decay * master
    return (master - learn_rate * update, first, variance)

def reference(query_grads, merge_grads, query_accum, merge_accum, query_master, merge_master, query_moment, merge_moment, query_second, merge_second):
    query_total = query_accum + lax.optimization_barrier(jnp.sum(query_grads.astype(jnp.float32), axis=0))
    merge_total = merge_accum + lax.optimization_barrier(jnp.sum(merge_grads.astype(jnp.float32), axis=0))
    sumsq = jnp.sum(query_total * query_total) + jnp.sum(merge_total * merge_total)
    clip = jnp.minimum(1.0, lax.rsqrt(sumsq / float(ENTRIES) + 1e-06))
    query_shard, query_first, query_variance = adamw(query_total, clip, query_master, query_moment, query_second)
    merge_shard, merge_first, merge_variance = adamw(merge_total, clip, merge_master, merge_moment, merge_second)
    return (query_shard.astype(jnp.bfloat16), merge_shard.astype(jnp.bfloat16), query_shard, merge_shard, query_first, merge_first, query_variance, merge_variance)
```

```python
import functools

import jax
import jax.numpy as jnp
from jax import lax
from jax.experimental import pallas as pl
from jax.experimental.pallas import tpu as pltpu
from jax.sharding import PartitionSpec as P

STEP = 10
ENTRIES = 29360128


beta_one = 0.9
beta_two = 0.95
learn_rate = 0.002
weight_decay = 0.1
adam_eps = 1e-08

CHUNKS = 8
ROWS = 16
CORES = 2
ORDER = (3, 1, 2, 0)
MESH_IDS = pl.DeviceIdType.MESH


def adamw(total, clip, master, moment, second):
    scaled = clip * total
    first = beta_one * moment + (1.0 - beta_one) * scaled
    variance = beta_two * second + (1.0 - beta_two) * scaled * scaled
    corr_one = 1.0 - beta_one**STEP
    corr_two = 1.0 - beta_two**STEP
    update = first / corr_one / (jnp.sqrt(variance / corr_two) + adam_eps) + weight_decay * master
    return (master - learn_rate * update, first, variance)


def step_kernel(
    n_mp,
    grads_q, grads_m, accum_q, accum_m, master_q, master_m, moment_q, moment_m, second_q, second_m,
    weight_q, weight_m, shard_q, shard_m, first_q, first_m, variance_q, variance_m,
    near_q, near_m, far_q, far_m, part_q, part_m, came_q, came_m,
    total_q, total_m, mast_q, mast_m, mom_q, mom_m, sec_q, sec_m,
    squares_q, squares_m, tile, tiles,
    local_sem, send_sem, recv_sem, tile_send, tile_recv, relay_sem,
):
    me = lax.axis_index("dp")
    mp = lax.axis_index("mp")
    low = me + 1 - 2 * (me % 2)
    high = (me + 2) % 4
    both = 3 - me

    q = dict(
        tag=0, grads=grads_q, one=low, two=high, near=near_q, far=far_q, part=part_q, came=came_q,
        total=total_q, master=mast_q, moment=mom_q, second=sec_q, squares=squares_q,
        weight=weight_q, shard=shard_q, first=first_q, variance=variance_q,
        fetch=((accum_q, total_q), (master_q, mast_q), (moment_q, mom_q), (second_q, sec_q)),
    )
    m = dict(
        tag=1, grads=grads_m, one=high, two=low, near=near_m, far=far_m, part=part_m, came=came_m,
        total=total_m, master=mast_m, moment=mom_m, second=sec_m, squares=squares_m,
        weight=weight_m, shard=shard_m, first=first_m, variance=variance_m,
        fetch=((accum_m, total_m), (master_m, mast_m), (moment_m, mom_m), (second_m, sec_m)),
    )
    sides = (q, m)
    for t in sides:
        t["rows"], t["cols"] = t["total"].shape
        t["step"] = t["rows"] // CHUNKS

    def block(t, ref, owner, start, size):
        if t["tag"] == 0:
            return ref.at[pl.ds(pl.multiple_of(owner * t["rows"] + start, ROWS), size), :]
        return ref.at[
            pl.ds(pl.multiple_of(start, ROWS), size),
            pl.ds(pl.multiple_of(owner * t["cols"], 128), t["cols"]),
        ]

    def chunk(t, c):
        return pl.ds(pl.multiple_of(c * t["step"], ROWS), t["step"])

    def remote(src, dst, send, recv, peer):
        return pltpu.make_async_remote_copy(
            src_ref=src, dst_ref=dst, send_sem=send, recv_sem=recv,
            device_id=(peer, mp), device_id_type=MESH_IDS,
        )

    local = []
    for t in sides:
        pairs = [
            (block(t, t["grads"], t["two"], 0, t["rows"]), t["near"].at[0]),
            (block(t, t["grads"], me, 0, t["rows"]), t["near"].at[1]),
        ] + list(t["fetch"])
        t["local"] = []
        for i, (src, dst) in enumerate(pairs):
            t["local"].append(pltpu.make_async_copy(src, dst, local_sem.at[t["tag"], i]))
        local.append(t["local"])
    for i in range(6):
        for t in sides:
            t["local"][i].start()

    lines, pair = n_mp // CORES, mp % CORES
    line = mp // CORES
    near = [(low, mp), (high, mp)]
    near += [(me, line * CORES + (pair + k) % CORES) for k in range(1, CORES)]
    up, down = line + 1 < lines, line > 0
    count = len(near) + up.astype(jnp.int32) + down.astype(jnp.int32)

    def greet(sem):
        for peer in near:
            pl.semaphore_signal(sem, inc=1, device_id=peer, device_id_type=MESH_IDS)

        @pl.when(up)
        def _():
            pl.semaphore_signal(sem, inc=1, device_id=(me, mp + CORES), device_id_type=MESH_IDS)

        @pl.when(down)
        def _():
            pl.semaphore_signal(sem, inc=1, device_id=(me, mp - CORES), device_id_type=MESH_IDS)

    barrier = pltpu.get_barrier_semaphore()
    greet(barrier)
    pl.semaphore_wait(barrier, count)
    hops = relay_sem.shape[0]
    others = [((me + i) % 4, (mp + k) % n_mp) for i in ORDER for k in range(n_mp) if i + k > 0]

    def first_copy(t, half, c):
        owner = both if half == 0 else t["one"]
        return remote(
            block(t, t["grads"], owner, c * t["step"], t["step"]),
            t["far"].at[half, chunk(t, c)],
            send_sem.at[t["tag"], half], recv_sem.at[t["tag"], half, c], t["one"],
        )

    def second_copy(t, c):
        return remote(
            t["part"].at[chunk(t, c)], t["came"].at[chunk(t, c)],
            send_sem.at[t["tag"], 2], recv_sem.at[t["tag"], 2, c], t["two"],
        )

    for half in range(2):
        @pl.loop(0, CHUNKS)
        def _(c):
            for t in sides:
                first_copy(t, half, c).start()

    def over_rows(t, c, body):
        @pl.loop(0, t["step"] // ROWS)
        def _(r):
            body(pl.ds(pl.multiple_of(c * t["step"] + r * ROWS, ROWS), ROWS))

    for i in range(hops):
        greet(relay_sem.at[i])
        pl.semaphore_wait(relay_sem.at[i], count)

    for t in sides:
        t["local"][0].wait()

    @pl.loop(0, CHUNKS)
    def _(c):
        for t in sides:
            first_copy(t, 0, c).wait_recv()

            def add(rows, t=t):
                both_terms = t["near"][0, rows, :].astype(jnp.float32) + t["far"][0, rows, :].astype(jnp.float32)
                t["part"][rows, :] = both_terms.astype(jnp.bfloat16)

            over_rows(t, c, add)
            second_copy(t, c).start()

    for t in sides:
        for i in range(1, 6):
            t["local"][i].wait()
        t["squares"][...] = jnp.zeros_like(t["squares"])

    @pl.loop(0, CHUNKS)
    def _(c):
        for t in sides:
            first_copy(t, 1, c).wait_recv()
            second_copy(t, c).wait_recv()

            def add(rows, t=t):
                own = t["near"][1, rows, :].astype(jnp.float32) + t["far"][1, rows, :].astype(jnp.float32)
                total = t["total"][rows, :] + (own + t["came"][rows, :].astype(jnp.float32))
                t["total"][rows, :] = total
                t["squares"][...] += total * total

            over_rows(t, c, add)

    lanes = tile.shape[1]
    local_squares = jnp.zeros((8, lanes), jnp.float32)
    for t in sides:
        for r in range(ROWS // 8):
            for c in range(t["cols"] // lanes):
                local_squares += t["squares"][r * 8 : (r + 1) * 8, c * lanes : (c + 1) * lanes]
    tile[...] = jnp.sum(local_squares, axis=0, keepdims=True)
    tile_copies = [
        pltpu.make_async_remote_copy(
            src_ref=tile, dst_ref=tiles.at[i], send_sem=tile_send, recv_sem=tile_recv,
            device_id=peer, device_id_type=MESH_IDS,
        )
        for i, peer in enumerate(others)
    ]
    for copy in tile_copies:
        copy.start()
    gathered = tile[...]
    pltpu.make_async_copy(tiles, tiles, tile_recv).wait()
    for i in range(len(others)):
        gathered += tiles[i]
    sumsq = jnp.full(tile.shape, jnp.sum(gathered), jnp.float32)
    clip = jnp.max(jnp.minimum(1.0, lax.rsqrt(sumsq / float(ENTRIES) + 1e-06)))

    def own_copy(t, way, c):
        peer = t["one"] if way == 0 else t["two"]
        ref = block(t, t["weight"], me, c * t["step"], t["step"])
        return remote(
            ref, ref, send_sem.at[t["tag"], 3 + way], recv_sem.at[t["tag"], way, c], peer
        )

    def passed_copy(t, c):
        ref = block(t, t["weight"], t["two"], c * t["step"], t["step"])
        return remote(
            ref, ref, send_sem.at[t["tag"], 5], recv_sem.at[t["tag"], 2, c], t["one"]
        )

    @pl.loop(0, CHUNKS)
    def _(c):
        for t in sides:
            def update(rows, t=t):
                shard, first, variance = adamw(
                    t["total"][rows, :], clip, t["master"][rows, :], t["moment"][rows, :], t["second"][rows, :]
                )
                t["shard"][rows, :] = shard
                t["first"][rows, :] = first
                t["variance"][rows, :] = variance
                if t["tag"] == 0:
                    at = pl.ds(pl.multiple_of(me * t["rows"] + rows.start, ROWS), ROWS)
                    t["weight"][at, :] = shard.astype(jnp.bfloat16)
                else:
                    at = pl.ds(pl.multiple_of(me * t["cols"], 128), t["cols"])
                    t["weight"][rows, at] = shard.astype(jnp.bfloat16)

            over_rows(t, c, update)
            own_copy(t, 1, c).start()
            own_copy(t, 0, c).start()

    @pl.loop(0, CHUNKS)
    def _(c):
        for t in sides:
            own_copy(t, 1, c).wait_recv()
            passed_copy(t, c).start()

    @pl.loop(0, CHUNKS)
    def _(c):
        for t in sides:
            own_copy(t, 0, c).wait_recv()
            passed_copy(t, c).wait_recv()

    for t in sides:
        for i in range(6):
            whole = t["part"]
            pltpu.make_async_copy(whole, whole, send_sem.at[t["tag"], i]).wait()
    pltpu.make_async_copy(tiles, tiles, tile_send).wait()


def store_kernel(*refs):
    sem = refs[-1]
    copies = [pltpu.make_async_copy(refs[i], refs[8 + i], sem.at[i]) for i in range(8)]
    for copy in copies:
        copy.start()
    for copy in copies:
        copy.wait()


def square_step(n_mp, *args):
    grads_q, grads_m = args[0][0, 0], args[1][0, 0]
    shards = [a[0] for a in args[2:]]
    shape_q, shape_m = shards[0].shape, shards[1].shape
    f32, bf16 = jnp.float32, jnp.bfloat16
    wide = dict(zip("qm", (shape_q, shape_m)))
    outs = [(grads_q.shape, bf16), (grads_m.shape, bf16)] + [(wide[k], f32) for k in "qmqmqm"]
    scratch = []
    for lead in ((2,), (2,), (), ()):
        scratch += [pltpu.VMEM(lead + wide[k], bf16) for k in "qm"]
    for _ in range(4):
        scratch += [pltpu.VMEM(wide[k], f32) for k in "qm"]
    scratch += [pltpu.VMEM((ROWS, wide[k][1]), f32) for k in "qm"]
    dma = pltpu.SemaphoreType.DMA
    scratch += [
        pltpu.VMEM((1, 128), f32),
        pltpu.VMEM((4 * n_mp - 1, 1, 128), f32),
        dma((2, 6)),
        dma((2, 6)),
        dma((2, 3, CHUNKS)),
        dma(()),
        dma(()),
        pltpu.SemaphoreType.REGULAR((max(n_mp // CORES, 1) + 1,)),
    ]
    results = pl.pallas_call(
        functools.partial(step_kernel, n_mp),
        out_shape=[OUT_SPACE(s, d) for s, d in outs],
        in_specs=[pl.BlockSpec(memory_space=pltpu.HBM)] * 10,
        out_specs=[pl.BlockSpec(memory_space=pltpu.VMEM)] * 8,
        scratch_shapes=scratch,
        compiler_params=pltpu.CompilerParams(
            collective_id=0, has_side_effects=True, vmem_limit_bytes=VMEM_LIMIT
        ),
    )(grads_q, grads_m, *shards)
    stored = pl.pallas_call(
        store_kernel,
        out_shape=[jax.ShapeDtypeStruct(s, d) for s, d in outs],
        in_specs=[pl.BlockSpec(memory_space=pltpu.VMEM)] * 8,
        out_specs=[pl.BlockSpec(memory_space=pltpu.HBM)] * 8,
        scratch_shapes=[dma((8,))],
        compiler_params=pltpu.CompilerParams(vmem_limit_bytes=1024 * 1024),
    )(*[pltpu.with_memory_space_constraint(r, pltpu.VMEM) for r in results])
    return tuple(r[None] for r in stored)


OUT_SPACE = pltpu.VMEM
VMEM_LIMIT = 40 * 1024 * 1024


def on_device(
    query_grads,
    merge_grads,
    query_accum,
    merge_accum,
    query_master,
    merge_master,
    query_moment,
    merge_moment,
    query_second,
    merge_second,
):
    query_sum, merge_sum = (
        lax.psum_scatter(
            query_grads[0].astype(jnp.float32).astype(jnp.bfloat16),
            "dp",
            scatter_dimension=1,
            tiled=True,
        ).astype(jnp.float32),
        lax.psum_scatter(
            merge_grads[0].astype(jnp.float32).astype(jnp.bfloat16),
            "dp",
            scatter_dimension=2,
            tiled=True,
        ).astype(jnp.float32),
    )
    query_total = query_accum + query_sum
    merge_total = merge_accum + merge_sum
    local_squares = jnp.sum(query_total * query_total) + jnp.sum(merge_total * merge_total)
    sumsq = lax.psum(local_squares, ("dp", "mp"))
    clip = jnp.minimum(1.0, lax.rsqrt(sumsq / float(ENTRIES) + 1e-06))
    query_shard, query_first, query_variance = adamw(
        query_total, clip, query_master, query_moment, query_second
    )
    merge_shard, merge_first, merge_variance = adamw(
        merge_total, clip, merge_master, merge_moment, merge_second
    )
    query_weight, merge_weight = (
        lax.all_gather(query_shard.astype(jnp.bfloat16), "dp", axis=1, tiled=True),
        lax.all_gather(merge_shard.astype(jnp.bfloat16), "dp", axis=2, tiled=True),
    )
    return (
        query_weight,
        merge_weight,
        query_shard,
        merge_shard,
        query_first,
        merge_first,
        query_variance,
        merge_variance,
    )


def solution(mesh):
    square = mesh.shape["dp"] == 4 and mesh.shape["mp"] % CORES == 0
    body = functools.partial(square_step, mesh.shape["mp"]) if square else on_device
    return jax.shard_map(
        body,
        mesh=mesh,
        in_specs=(
            P("dp", None, None, "mp"),
            P("dp", None, "mp", None),
            P(None, "dp", "mp"),
            P(None, "mp", "dp"),
            P(None, "dp", "mp"),
            P(None, "mp", "dp"),
            P(None, "dp", "mp"),
            P(None, "mp", "dp"),
            P(None, "dp", "mp"),
            P(None, "mp", "dp"),
        ),
        out_specs=(
            P(None, None, "mp"),
            P(None, "mp", None),
            P(None, "dp", "mp"),
            P(None, "mp", "dp"),
            P(None, "dp", "mp"),
            P(None, "mp", "dp"),
            P(None, "dp", "mp"),
            P(None, "mp", "dp"),
        ),
        check_vma=False,
    )
```

```python
import functools

import jax
import jax.numpy as jnp
from jax import lax
from jax.experimental import pallas as pl
from jax.experimental.pallas import tpu as pltpu
from jax.sharding import PartitionSpec as P

STEP = 10
ENTRIES = 29360128


beta_one = 0.9
beta_two = 0.95
learn_rate = 0.002
weight_decay = 0.1
adam_eps = 1e-08

CHUNKS = 8
ROWS = 16
CORES = 2
HELPERS = 2
ORDER = (3, 1, 2, 0)
MESH_IDS = pl.DeviceIdType.MESH


def adamw(total, clip, master, moment, second):
    scaled = clip * total
    first = beta_one * moment + (1.0 - beta_one) * scaled
    variance = beta_two * second + (1.0 - beta_two) * scaled * scaled
    corr_one = 1.0 - beta_one**STEP
    corr_two = 1.0 - beta_two**STEP
    update = first / corr_one / (jnp.sqrt(variance / corr_two) + adam_eps) + weight_decay * master
    return (master - learn_rate * update, first, variance)


def step_kernel(
    n_mp,
    grads_q, grads_m, accum_q, accum_m, master_q, master_m, moment_q, moment_m, second_q, second_m,
    weight_q, weight_m, shard_q, shard_m, first_q, first_m, variance_q, variance_m,
    near_q, near_m, far_q, far_m, part_q, part_m, came_q, came_m,
    total_q, total_m, mast_q, mast_m, mom_q, mom_m, sec_q, sec_m,
    squares_q, squares_m, tile, tiles, early_q, early_m, climb_q, climb_m, cross_q, cross_m,
    local_sem, send_sem, recv_sem, tile_send, tile_recv, relay_sem, early_sem, climb_sem, cross_sem, hop_sem,
):
    me = lax.axis_index("dp")
    mp = lax.axis_index("mp")
    low = me + 1 - 2 * (me % 2)
    high = (me + 2) % 4
    both = 3 - me

    q = dict(
        tag=0, grads=grads_q, one=low, two=high, near=near_q, far=far_q, part=part_q, came=came_q,
        total=total_q, master=mast_q, moment=mom_q, second=sec_q, squares=squares_q, early=early_q, climb=climb_q, cross=cross_q,
        weight=weight_q, shard=shard_q, first=first_q, variance=variance_q,
        fetch=((accum_q, total_q), (master_q, mast_q), (moment_q, mom_q), (second_q, sec_q)),
    )
    m = dict(
        tag=1, grads=grads_m, one=high, two=low, near=near_m, far=far_m, part=part_m, came=came_m,
        total=total_m, master=mast_m, moment=mom_m, second=sec_m, squares=squares_m, early=early_m, climb=climb_m, cross=cross_m,
        weight=weight_m, shard=shard_m, first=first_m, variance=variance_m,
        fetch=((accum_m, total_m), (master_m, mast_m), (moment_m, mom_m), (second_m, sec_m)),
    )
    sides = (q, m)
    for t in sides:
        t["rows"], t["cols"] = t["total"].shape
        t["step"] = t["rows"] // CHUNKS

    def block(t, ref, owner, start, size):
        if t["tag"] == 0:
            return ref.at[pl.ds(pl.multiple_of(owner * t["rows"] + start, ROWS), size), :]
        return ref.at[
            pl.ds(pl.multiple_of(start, ROWS), size),
            pl.ds(pl.multiple_of(owner * t["cols"], 128), t["cols"]),
        ]

    def chunk(t, c):
        return pl.ds(pl.multiple_of(c * t["step"], ROWS), t["step"])

    def remote(src, dst, send, recv, peer):
        return pltpu.make_async_remote_copy(
            src_ref=src, dst_ref=dst, send_sem=send, recv_sem=recv,
            device_id=(peer, mp), device_id_type=MESH_IDS,
        )

    early = []
    for t in sides:
        copy = pltpu.make_async_copy(
            block(t, t["grads"], both, 0, t["step"]), t["early"], early_sem.at[t["tag"]]
        )
        copy.start()
        early.append(copy)

    for t in sides:
        pairs = [
            (block(t, t["grads"], t["two"], 0, t["rows"]), t["near"].at[0]),
            (block(t, t["grads"], me, 0, t["rows"]), t["near"].at[1]),
        ] + list(t["fetch"])
        t["local"] = []
        for i, (src, dst) in enumerate(pairs):
            t["local"].append(pltpu.make_async_copy(src, dst, local_sem.at[t["tag"], i]))

    lines, pair = n_mp // CORES, mp % CORES
    line = mp // CORES
    near = [(low, mp), (high, mp)]
    near += [(me, line * CORES + (pair + k) % CORES) for k in range(1, CORES)]
    up, down = line + 1 < lines, line > 0
    count = len(near) + up.astype(jnp.int32) + down.astype(jnp.int32)

    def at_line(place):
        return (me, place * CORES + pair)

    def greet(sem):
        for peer in near:
            pl.semaphore_signal(sem, inc=1, device_id=peer, device_id_type=MESH_IDS)

        @pl.when(up)
        def _():
            pl.semaphore_signal(sem, inc=1, device_id=(me, mp + CORES), device_id_type=MESH_IDS)

        @pl.when(down)
        def _():
            pl.semaphore_signal(sem, inc=1, device_id=(me, mp - CORES), device_id_type=MESH_IDS)

    barrier = pltpu.get_barrier_semaphore()
    greet(barrier)
    pl.semaphore_wait(barrier, count)
    hops = relay_sem.shape[0]
    others = [((me + i) % 4, (mp + k) % n_mp) for i in ORDER for k in range(n_mp) if i + k > 0]

    def first_copy(t, half, c):
        owner = both if half == 0 else t["one"]
        return remote(
            block(t, t["grads"], owner, c * t["step"], t["step"]),
            t["far"].at[half, chunk(t, c)],
            send_sem.at[t["tag"], half], recv_sem.at[t["tag"], half, c], t["one"],
        )

    def second_copy(t, c):
        return remote(
            t["part"].at[chunk(t, c)], t["came"].at[chunk(t, c)],
            send_sem.at[t["tag"], 2], recv_sem.at[t["tag"], 2, c], t["two"],
        )

    def early_copy(t):
        return remote(
            t["early"], t["far"].at[0, chunk(t, 0)],
            send_sem.at[t["tag"], 0], recv_sem.at[t["tag"], 0, 0], t["one"],
        )

    for t in sides:
        early[t["tag"]].wait()
        early_copy(t).start()
    for half in range(2):
        @pl.loop(1 - half, CHUNKS)
        def _(c):
            for t in sides:
                first_copy(t, half, c).start()
    for i in range(6):
        for t in sides:
            t["local"][i].start()

    def over_rows(t, c, body):
        @pl.loop(0, t["step"] // ROWS)
        def _(r):
            body(pl.ds(pl.multiple_of(c * t["step"] + r * ROWS, ROWS), ROWS))

    for i in range(hops):
        greet(relay_sem.at[i])
        pl.semaphore_wait(relay_sem.at[i], count)

    for t in sides:
        t["local"][0].wait()

    @pl.loop(0, CHUNKS)
    def _(c):
        for t in sides:
            first_copy(t, 0, c).wait_recv()

            def add(rows, t=t):
                both_terms = t["near"][0, rows, :].astype(jnp.float32) + t["far"][0, rows, :].astype(jnp.float32)
                t["part"][rows, :] = both_terms.astype(jnp.bfloat16)

            over_rows(t, c, add)
            second_copy(t, c).start()

    for t in sides:
        for i in range(1, 6):
            t["local"][i].wait()
        t["squares"][...] = jnp.zeros_like(t["squares"])

    @pl.loop(0, CHUNKS)
    def _(c):
        for t in sides:
            first_copy(t, 1, c).wait_recv()
            second_copy(t, c).wait_recv()

            def add(rows, t=t):
                own = t["near"][1, rows, :].astype(jnp.float32) + t["far"][1, rows, :].astype(jnp.float32)
                total = t["total"][rows, :] + (own + t["came"][rows, :].astype(jnp.float32))
                t["total"][rows, :] = total
                t["squares"][...] += total * total

            over_rows(t, c, add)

    lanes = tile.shape[1]
    local_squares = jnp.zeros((8, lanes), jnp.float32)
    for t in sides:
        for r in range(ROWS // 8):
            for c in range(t["cols"] // lanes):
                local_squares += t["squares"][r * 8 : (r + 1) * 8, c * lanes : (c + 1) * lanes]
    tile[...] = jnp.sum(local_squares, axis=0, keepdims=True)
    tile_copies = [
        pltpu.make_async_remote_copy(
            src_ref=tile, dst_ref=tiles.at[i], send_sem=tile_send, recv_sem=tile_recv,
            device_id=peer, device_id_type=MESH_IDS,
        )
        for i, peer in enumerate(others)
    ]
    for copy in tile_copies:
        copy.start()
    gathered = tile[...]
    pltpu.make_async_copy(tiles, tiles, tile_recv).wait()
    for i in range(len(others)):
        gathered += tiles[i]
    sumsq = jnp.full(tile.shape, jnp.sum(gathered), jnp.float32)
    clip = jnp.max(jnp.minimum(1.0, lax.rsqrt(sumsq / float(ENTRIES) + 1e-06)))

    def own_copy(t, way, c):
        peer = t["one"] if way == 0 else t["two"]
        ref = block(t, t["weight"], me, c * t["step"], t["step"])
        return remote(
            ref, ref, send_sem.at[t["tag"], 3 + way], recv_sem.at[t["tag"], way, c], peer
        )

    def passed_copy(t, c):
        ref = block(t, t["weight"], t["two"], c * t["step"], t["step"])
        return remote(
            ref, ref, send_sem.at[t["tag"], 5], recv_sem.at[t["tag"], 2, c], t["one"]
        )

    helpers = tuple(range(lines - HELPERS, lines)) if lines > HELPERS + 1 else ()

    def span(t, i):
        small = t["step"] // HELPERS // ROWS * ROWS
        return i * small, small if i < HELPERS - 1 else t["step"] - i * small

    def piece(t, ref, owner, i):
        return block(t, ref, owner, *span(t, i))

    def slot(t, name, i):
        return t[name].at[pl.ds(0, span(t, i)[1])]

    def climb_copy(t, i, place):
        return pltpu.make_async_remote_copy(
            src_ref=piece(t, t["weight"], me, i), dst_ref=slot(t, "climb", i),
            send_sem=send_sem.at[t["tag"], 3], recv_sem=climb_sem.at[t["tag"]],
            device_id=at_line(place), device_id_type=MESH_IDS,
        )

    def cross_copy(t, i):
        return remote(
            slot(t, "climb", i), slot(t, "cross", i),
            hop_sem.at[t["tag"], 0], cross_sem.at[t["tag"]], t["one"],
        )

    def drop_copy(t, i):
        return pltpu.make_async_remote_copy(
            src_ref=slot(t, "cross", i), dst_ref=piece(t, t["weight"], t["one"], i),
            send_sem=hop_sem.at[t["tag"], 1], recv_sem=recv_sem.at[t["tag"], 0, 0],
            device_id=at_line(0), device_id_type=MESH_IDS,
        )

    @pl.loop(0, CHUNKS)
    def _(c):
        for t in sides:
            def update(rows, t=t):
                shard, first, variance = adamw(
                    t["total"][rows, :], clip, t["master"][rows, :], t["moment"][rows, :], t["second"][rows, :]
                )
                t["shard"][rows, :] = shard
                t["first"][rows, :] = first
                t["variance"][rows, :] = variance
                if t["tag"] == 0:
                    at = pl.ds(pl.multiple_of(me * t["rows"] + rows.start, ROWS), ROWS)
                    t["weight"][at, :] = shard.astype(jnp.bfloat16)
                else:
                    at = pl.ds(pl.multiple_of(me * t["cols"], 128), t["cols"])
                    t["weight"][rows, at] = shard.astype(jnp.bfloat16)

            over_rows(t, c, update)
            own_copy(t, 1, c).start()
            if not helpers:
                own_copy(t, 0, c).start()
            else:
                around = jnp.logical_and(c == 0, line == 0)

                @pl.when(around)
                def _():
                    for i, place in enumerate(helpers):
                        climb_copy(t, i, place).start()

                @pl.when(jnp.logical_not(around))
                def _():
                    own_copy(t, 0, c).start()

    for i, place in enumerate(helpers):
        @pl.when(line == place)
        def _():
            for t in sides:
                climb_copy(t, i, place).wait_recv()
                cross_copy(t, i).start()

    @pl.loop(0, CHUNKS)
    def _(c):
        for t in sides:
            own_copy(t, 1, c).wait_recv()
            passed_copy(t, c).start()

    for i, place in enumerate(helpers):
        @pl.when(line == place)
        def _():
            for t in sides:
                cross_copy(t, i).wait_recv()
                drop_copy(t, i).start()
            for t in sides:
                cross_copy(t, i).wait_send()
                drop_copy(t, i).wait_send()

    @pl.loop(0, CHUNKS)
    def _(c):
        for t in sides:
            own_copy(t, 0, c).wait_recv()
            passed_copy(t, c).wait_recv()

    for t in sides:
        for i in range(6):
            whole = t["part"]
            pltpu.make_async_copy(whole, whole, send_sem.at[t["tag"], i]).wait()
    pltpu.make_async_copy(tiles, tiles, tile_send).wait()


def store_kernel(*refs):
    sem = refs[-1]
    copies = [pltpu.make_async_copy(refs[i], refs[8 + i], sem.at[i]) for i in range(8)]
    for copy in copies:
        copy.start()
    for copy in copies:
        copy.wait()


def square_step(n_mp, *args):
    grads_q, grads_m = args[0][0, 0], args[1][0, 0]
    shards = [a[0] for a in args[2:]]
    shape_q, shape_m = shards[0].shape, shards[1].shape
    f32, bf16 = jnp.float32, jnp.bfloat16
    wide = dict(zip("qm", (shape_q, shape_m)))
    outs = [(grads_q.shape, bf16), (grads_m.shape, bf16)] + [(wide[k], f32) for k in "qmqmqm"]
    scratch = []
    for lead in ((2,), (2,), (), ()):
        scratch += [pltpu.VMEM(lead + wide[k], bf16) for k in "qm"]
    for _ in range(4):
        scratch += [pltpu.VMEM(wide[k], f32) for k in "qm"]
    scratch += [pltpu.VMEM((ROWS, wide[k][1]), f32) for k in "qm"]
    dma = pltpu.SemaphoreType.DMA
    scratch += [
        pltpu.VMEM((1, 128), f32),
        pltpu.VMEM((4 * n_mp - 1, 1, 128), f32),
    ]
    for _ in range(3):
        scratch += [pltpu.VMEM((wide[k][0] // CHUNKS, wide[k][1]), bf16) for k in "qm"]
    scratch += [
        dma((2, 6)),
        dma((2, 6)),
        dma((2, 3, CHUNKS)),
        dma(()),
        dma(()),
        pltpu.SemaphoreType.REGULAR((max(n_mp // CORES, 1) + 1,)),
        dma((2,)),
        dma((2,)),
        dma((2,)),
        dma((2, 2)),
    ]
    results = pl.pallas_call(
        functools.partial(step_kernel, n_mp),
        out_shape=[OUT_SPACE(s, d) for s, d in outs],
        in_specs=[pl.BlockSpec(memory_space=pltpu.HBM)] * 10,
        out_specs=[pl.BlockSpec(memory_space=pltpu.VMEM)] * 8,
        scratch_shapes=scratch,
        compiler_params=pltpu.CompilerParams(
            collective_id=0, has_side_effects=True, vmem_limit_bytes=VMEM_LIMIT
        ),
    )(grads_q, grads_m, *shards)
    stored = pl.pallas_call(
        store_kernel,
        out_shape=[jax.ShapeDtypeStruct(s, d) for s, d in outs],
        in_specs=[pl.BlockSpec(memory_space=pltpu.VMEM)] * 8,
        out_specs=[pl.BlockSpec(memory_space=pltpu.HBM)] * 8,
        scratch_shapes=[dma((8,))],
        compiler_params=pltpu.CompilerParams(vmem_limit_bytes=1024 * 1024),
    )(*[pltpu.with_memory_space_constraint(r, pltpu.VMEM) for r in results])
    return tuple(r[None] for r in stored)


OUT_SPACE = pltpu.VMEM
VMEM_LIMIT = 40 * 1024 * 1024


def on_device(
    query_grads,
    merge_grads,
    query_accum,
    merge_accum,
    query_master,
    merge_master,
    query_moment,
    merge_moment,
    query_second,
    merge_second,
):
    query_sum, merge_sum = (
        lax.psum_scatter(
            query_grads[0].astype(jnp.float32).astype(jnp.bfloat16),
            "dp",
            scatter_dimension=1,
            tiled=True,
        ).astype(jnp.float32),
        lax.psum_scatter(
            merge_grads[0].astype(jnp.float32).astype(jnp.bfloat16),
            "dp",
            scatter_dimension=2,
            tiled=True,
        ).astype(jnp.float32),
    )
    query_total = query_accum + query_sum
    merge_total = merge_accum + merge_sum
    local_squares = jnp.sum(query_total * query_total) + jnp.sum(merge_total * merge_total)
    sumsq = lax.psum(local_squares, ("dp", "mp"))
    clip = jnp.minimum(1.0, lax.rsqrt(sumsq / float(ENTRIES) + 1e-06))
    query_shard, query_first, query_variance = adamw(
        query_total, clip, query_master, query_moment, query_second
    )
    merge_shard, merge_first, merge_variance = adamw(
        merge_total, clip, merge_master, merge_moment, merge_second
    )
    query_weight, merge_weight = (
        lax.all_gather(query_shard.astype(jnp.bfloat16), "dp", axis=1, tiled=True),
        lax.all_gather(merge_shard.astype(jnp.bfloat16), "dp", axis=2, tiled=True),
    )
    return (
        query_weight,
        merge_weight,
        query_shard,
        merge_shard,
        query_first,
        merge_first,
        query_variance,
        merge_variance,
    )


def solution(mesh):
    square = mesh.shape["dp"] == 4 and mesh.shape["mp"] % CORES == 0
    body = functools.partial(square_step, mesh.shape["mp"]) if square else on_device
    return jax.shard_map(
        body,
        mesh=mesh,
        in_specs=(
            P("dp", None, None, "mp"),
            P("dp", None, "mp", None),
            P(None, "dp", "mp"),
            P(None, "mp", "dp"),
            P(None, "dp", "mp"),
            P(None, "mp", "dp"),
            P(None, "dp", "mp"),
            P(None, "mp", "dp"),
            P(None, "dp", "mp"),
            P(None, "mp", "dp"),
        ),
        out_specs=(
            P(None, None, "mp"),
            P(None, "mp", None),
            P(None, "dp", "mp"),
            P(None, "mp", "dp"),
            P(None, "dp", "mp"),
            P(None, "mp", "dp"),
            P(None, "dp", "mp"),
            P(None, "mp", "dp"),
        ),
        check_vma=False,
    )
```
